256 devices in a mesh: seq: 64 (over y, z, core), layer: 4 (over x).
Axes of the slice: x: 4, y: 4, z: 8, core: 2. Of those that a mesh axis runs over, the one named last changes fastest.
Arguments:
- gradients: bfloat16 [16384, 4096], P('seq', 'layer'), may hold values from -6 to 6
- projection: bfloat16 [4096, 8192], P('layer', 'seq'), may hold values from -0.09375 to 0.09375
- queries: bfloat16 [256, 8192], P(None, 'seq'), may hold values from -6 to 6
Outputs:
- scores: float32 [16384, 256], P(('seq', 'layer'))
The draws below stay inside these ranges and needn't reach their ends.
All inputs are finite; a program needn't handle non-finite values.
Results may differ from the reference program's by a relative error of at most 0.0029.
Values may be sent and summed in bfloat16 or wider, within the bound.
No kernel may reach another device: no remote copies, remote signals or barrier semaphores. Data moves between devices by JAX's collectives and lax.ppermute only.
A program may use at most 128 MiB of HBM per device.

```python
import math
import jax
import jax.numpy as jnp
from jax import lax

FEAT = 4096
K = 8192
Q = 256
S = 16384


def level_of(own_key, extent, split, low, high):
    gain = 1.0
    for position, blocks in split:
        steps = jax.random.uniform(jax.random.fold_in(jax.random.fold_in(own_key, 6), position), (blocks,), jnp.float32, low / len(split), high / len(split))
        gain = gain * jnp.repeat(jnp.exp(steps), extent[position] // blocks).reshape((-1,) + (1,) * (len(extent) - 1 - position))
    return gain


def centred(key, extent, spread, bound, shards=(), held_as=jnp.bfloat16):
    factor_of = level_of(key, extent, shards, -0.22, 0.18) if shards else 1.0
    array = jax.random.normal(key, extent, jnp.float32) * spread * factor_of
    return jnp.minimum(jnp.maximum(array, -bound), bound).astype(held_as)


def setup_inputs(seed: int = 0) -> dict:
    keys = jax.random.split(jax.random.key(seed), 4)
    gradients = centred(keys[0], (S, FEAT), 1.0, 6.0, ((0, 64), (1, 4)))
    projection = centred(keys[1], (FEAT, K), FEAT ** -0.5, 0.09375, ((0, 4), (1, 64)))
    queries = centred(keys[2], (Q, K), 1.0, 6.0, ((1, 64),))
    return dict(gradients=gradients, projection=projection, queries=queries)


epsilon = 1e-06

def reference(gradients, projection, queries):
    sketch = jnp.dot(gradients, projection, preferred_element_type=jnp.float32).astype(jnp.bfloat16)
    sketch_wide = sketch.astype(jnp.float32)
    row_squares = lax.optimization_barrier(jnp.sum(sketch_wide * sketch_wide, axis=1))
    query_wide = queries.astype(jnp.float32)
    query_squares = lax.optimization_barrier(jnp.sum(query_wide * query_wide, axis=1))
    products = lax.dot_general(sketch, queries, (((1,), (1,)), ((), ())), preferred_element_type=jnp.float32)
    return math.sqrt(K) * products * lax.rsqrt(row_squares + epsilon)[:, None] * lax.rsqrt(query_squares + epsilon)[None, :]
```

```python
import math

import jax
import jax.numpy as jnp
from jax import lax
from jax.sharding import PartitionSpec as P

K = 8192
Y, Z, C, X = 4, 8, 2, 4
epsilon = 1e-06
bf16 = jnp.bfloat16
f32 = jnp.float32


def seq_shift(dy=0, dz=0, dc=0):
    pairs = []
    for y in range(Y):
        for z in range(Z):
            for c in range(C):
                there = (((y + dy) % Y) * Z + (z + dz) % Z) * C + (c + dc) % C
                pairs.append(((y * Z + z) * C + c, there))
    return pairs


def to_y(a, k):
    return lax.ppermute(a, "seq", seq_shift(dy=k))


def to_z(a, k):
    return lax.ppermute(a, "seq", seq_shift(dz=k))


def to_other_core(a):
    return lax.ppermute(a, "seq", seq_shift(dc=1))


def to_x(a, k):
    return lax.ppermute(a, "layer", [(i, (i + k) % X) for i in range(X)])


def dot(a, b):
    return jnp.dot(a, b, preferred_element_type=f32)


def ring4(a, shift, axis=0):
    up = shift(a, 1)
    down = shift(a, -1)
    half = a.shape[axis] // 2
    first = shift(lax.slice_in_dim(up, 0, half, axis=axis), 1)
    second = shift(lax.slice_in_dim(down, half, 2 * half, axis=axis), -1)
    return up, down, jnp.concatenate([first, second], axis=axis)


def reduce_to_x(parts):
    two, one, three, own = parts[2], parts[1], parts[3], parts[0]
    half = own.shape[1] // 2
    a_up = to_x(two[:, :half].astype(bf16), 1)
    a_down = to_x(two[:, half:].astype(bf16), -1)
    b_up = to_x(one[:, half:].astype(bf16), 1)
    b_down = to_x(three[:, :half].astype(bf16), -1)
    c_up = to_x((one[:, :half] + a_up.astype(f32)).astype(bf16), 1)
    c_down = to_x((three[:, half:] + a_down.astype(f32)).astype(bf16), -1)
    left = own[:, :half] + c_up.astype(f32) + b_down.astype(f32)
    right = own[:, half:] + b_up.astype(f32) + c_down.astype(f32)
    return left, right


def reduce_to_x_f32(parts):
    two, one, three, own = parts[2], parts[1], parts[3], parts[0]
    half = own.shape[1] // 2
    a_up = to_x(two[:, :half], 1)
    a_down = to_x(two[:, half:], -1)
    b_up = to_x(one[:, half:], 1)
    b_down = to_x(three[:, :half], -1)
    c_up = to_x(one[:, :half] + a_up, 1)
    c_down = to_x(three[:, half:] + a_down, -1)
    left = own[:, :half] + c_up + b_down
    right = own[:, half:] + b_up + c_down
    return jnp.concatenate([left, right], axis=1)


def shards(gradients, projection, queries):
    rows = gradients.shape[0] // X
    x = lax.axis_index("layer")
    core = lax.axis_index("seq") % C
    feats = projection.shape[0]

    twice = jnp.concatenate([gradients, gradients], axis=0)
    mine = lax.dynamic_slice_in_dim(twice, x * rows, X * rows, 0)

    both = jnp.concatenate([projection, queries], axis=0)
    chain = [both]
    up = down = both
    for step in range(3):
        up = to_z(up, 1)
        down = to_z(down, -1)
        chain += [up, down]
    half = both.shape[0] // 2
    chain.append(
        jnp.concatenate([to_z(up[:half], 1), to_z(down[half:], -1)], axis=0)
    )

    g_up, g_down, g_far = ring4(mine, to_y)
    own_core = [mine, g_up, g_down, g_far]
    other_core = [to_other_core(g) for g in own_core]
    blocks = own_core + other_core
    stacked = jnp.stack(blocks).reshape(2 * Y, X, rows, feats)

    columns = jnp.concatenate(chain, axis=1)
    proj, quer = columns[:feats], columns[feats:]

    part = lax.dot_general(
        proj, quer, (((1,), (1,)), ((), ())), preferred_element_type=f32
    )
    quer_wide = quer.astype(f32)
    squares = jnp.sum(quer_wide * quer_wide, axis=1)
    q = part.shape[1] // 2
    ext = jnp.concatenate([part, jnp.broadcast_to(squares[None], (8, 2 * q))], axis=0)
    keep = lax.dynamic_slice_in_dim(ext, core * q, q, 1)
    give = lax.dynamic_slice_in_dim(ext, (1 - core) * q, q, 1)
    keep = keep + to_other_core(give)
    w_up, w_down, w_far = ring4(keep, to_y)
    summed = (keep + w_far) + (w_up + w_down)
    other = to_other_core(summed)
    low = jnp.where(core == 0, summed, other)
    high = jnp.where(core == 0, other, summed)
    weights = jnp.concatenate([low, high], axis=1)
    query_squares = weights[feats]
    weights = weights[:feats]
    w_hi = weights.astype(bf16)
    w_lo = (weights - w_hi.astype(f32)).astype(bf16)
    prod = dot(mine, w_hi) + dot(mine, w_lo)
    products = reduce_to_x_f32([prod[d * rows : (d + 1) * rows] for d in range(X)])

    terms = [
        dot(stacked[:, d].reshape(2 * Y * rows, feats), proj) for d in range(X)
    ]
    left, right = reduce_to_x(terms)
    norms = jnp.sum(left * left, axis=1) + jnp.sum(right * right, axis=1)
    norms = norms.reshape(2, Y, rows)
    norms = norms[0] + to_other_core(norms[1])
    row_squares = (
        norms[0] + to_y(norms[1], -1) + to_y(norms[2], 1) + to_y(norms[3], 2)
    )
    return (
        math.sqrt(K)
        * products
        * lax.rsqrt(row_squares + epsilon)[:, None]
        * lax.rsqrt(query_squares + epsilon)[None, :]
    )


def solution(mesh):
    placed = (P("seq", "layer"), P("layer", "seq"), P(None, "seq"))
    return jax.shard_map(
        shards, mesh=mesh, in_specs=placed, out_specs=P(("seq", "layer"), None), check_vma=False
    )
```
